32 devices in a mesh: blk: 8 (over z, y), feat: 4 (over x, core).
Axes of the slice: x: 2, y: 2, z: 4, core: 2. Of those that a mesh axis runs over, the one named last changes fastest.
Arguments:
- node_feats: bfloat16 [65536, 256], P('blk', 'feat'), may hold values from -6 to 6
- tile_rows: int32 [64, 128], P('blk'), may hold values from 0 to 63, as said below
- tile_cols: int32 [64, 128], P('blk'), may hold values from 0 to 63, as said below
- tile_values: bfloat16 [64, 128, 128, 128], P('blk'), may hold values from 0 to 0.1, as said below
- eps_self: float32 [1], replicated, may hold values from -0.5 to 0.5
- w_one: bfloat16 [256, 256], P(None, 'feat'), may hold values from -0.375 to 0.375
- b_one: bfloat16 [256], P('feat'), may hold values from -3 to 3
- w_two: bfloat16 [256, 256], P('feat'), may hold values from -0.375 to 0.375
- b_two: bfloat16 [256], P('feat'), may hold values from -3 to 3
Outputs:
- layer_out: bfloat16 [65536, 256], P('blk', 'feat')
The draws below stay inside these ranges and needn't reach their ends.
Inputs may be any that keep to these rules, and one draw needn't show every extreme that they name: `tile_rows`: every entry names a row of tiles inside a node block: 0 to 63; within one row of the lists no pair (tile_rows, tile_cols) repeats; every row of tiles of every node block holds at least one nonzero tile. `tile_cols`: every entry names a column of tiles inside a source block: 0 to 63; every node block has exactly 128 tiles in each source block; every column of tiles of every source block is used by at least one node block. `tile_values`: edge weights are 0 or positive and below 0.1.
All inputs are finite; a program needn't handle non-finite values.
Results may differ from the reference program's by a relative error of at most 0.01.
Values may be sent and summed in bfloat16 or wider, within the bound.
A program may use at most 192 MiB of HBM per device.

```python
import jax
import jax.numpy as jnp
from jax import lax

FEATS = 256
TILE = 128
NODE_DEV = 8192
NODES = 65536
SLOTS = 128
N_BLK = 8


def bit_weight(values):
    total = jnp.zeros_like(values)
    for place in range(16):
        total = total + values // 2 ** place % 2
    return total


def tile_choice(key):
    row_tiles = NODE_DEV // TILE
    options = row_tiles * row_tiles
    spread = (row_tiles + N_BLK - 1) // N_BLK
    subkey = jax.random.fold_in(key, 911)
    noise = jax.random.randint(subkey, (N_BLK * N_BLK, options), 0, 65536, dtype=jnp.int32)
    option = jnp.arange(options, dtype=jnp.int32)
    opt_row = option // row_tiles
    opt_col = option % row_tiles
    weight_bits = bit_weight(opt_row) + bit_weight(opt_col)
    pair_ids = jnp.arange(N_BLK * N_BLK, dtype=jnp.int32)
    owner = pair_ids // N_BLK
    source = pair_ids % N_BLK
    offset = (opt_col[None, :] - owner[:, None] * spread) % row_tiles
    forced = (offset < spread) & (opt_row[None, :] == (source[:, None] * spread + offset) % row_tiles)
    base = jnp.right_shift(noise, (weight_bits // 3)[None, :])
    scores = jnp.where(forced, 65536, base) * options + option[None, :]
    ranked, chosen = lax.top_k(scores, SLOTS)
    return chosen.astype(jnp.int32)


def draw_tile_rows(key, part):
    return tile_choice(key) // (NODE_DEV // TILE)


def draw_tile_cols(key, part):
    return tile_choice(key) % (NODE_DEV // TILE)


def draw_tile_values(key, part):
    shape = (N_BLK * N_BLK, SLOTS, TILE, TILE)
    edges = (jax.random.randint(jax.random.fold_in(key, 5), shape, 0, 8, dtype=jnp.int32) == 0).astype(jnp.float32)
    return (edges * 0.0625).astype(jnp.bfloat16)


def block_scale(key, extent, cuts, low, top_value):
    factor_of, own = 1.0, jax.random.fold_in(key, 6)
    for dim, shards_of in cuts:
        steps = jnp.exp(jax.random.uniform(jax.random.fold_in(own, dim), (shards_of,), jnp.float32, low / len(cuts), top_value / len(cuts)))
        factor_of = factor_of * jnp.repeat(steps, extent[dim] // shards_of).reshape([-1 if axis == dim else 1 for axis in range(len(extent))])
    return factor_of


def gaussian(rng, dims, scale, reach, shards=(), kind=jnp.bfloat16):
    values = scale * jax.random.normal(rng, dims, jnp.float32)
    if shards:
        values = values * block_scale(rng, dims, shards, -0.22, 0.18)
    return jnp.clip(values, -reach, reach).astype(kind)


def setup_inputs(seed: int = 0) -> dict:
    splits = jax.random.split(jax.random.key(seed), 10)
    return {
        "node_feats": gaussian(splits[0], (NODES, FEATS), 1.0, 6.0, ((0, 8), (1, 4))),
        "tile_rows": draw_tile_rows(jax.random.fold_in(splits[9], 71), 0),
        "tile_cols": draw_tile_cols(jax.random.fold_in(splits[9], 71), 0),
        "tile_values": draw_tile_values(jax.random.fold_in(splits[9], 71), 0),
        "eps_self": jnp.clip(jax.random.uniform(splits[4], (1,), jnp.float32, -0.5, 0.5), -0.5, 0.5),
        "w_one": gaussian(splits[5], (FEATS, FEATS), FEATS ** -0.5, 0.375, ((1, 4),)),
        "b_one": gaussian(splits[6], (FEATS,), 0.5, 3.0, ((0, 4),)),
        "w_two": gaussian(splits[7], (FEATS, FEATS), FEATS ** -0.5, 0.375, ((0, 4),)),
        "b_two": gaussian(splits[8], (FEATS,), 0.5, 3.0, ((0, 4),)),
    }


def reference(node_feats, tile_rows, tile_cols, tile_values, eps_self, w_one, b_one, w_two, b_two):
    row_tiles = NODE_DEV // TILE
    sources = node_feats.astype(jnp.float32).reshape(N_BLK, row_tiles, TILE, FEATS)
    rows_all = tile_rows.reshape(N_BLK, N_BLK, SLOTS)
    cols_all = tile_cols.reshape(N_BLK, N_BLK, SLOTS)
    vals_all = tile_values.reshape(N_BLK, N_BLK, SLOTS, TILE, TILE)
    block_ids = jnp.arange(N_BLK, dtype=jnp.int32)
    tile_ids = jnp.arange(row_tiles, dtype=jnp.int32)

    def one_block(packed):
        row_ids, col_ids, tile_vals = packed
        picked = sources[block_ids[:, None], col_ids]
        products = jnp.einsum("skij,skjh->skih", tile_vals.astype(jnp.float32), picked)
        row_marks = (row_ids[:, :, None] == tile_ids[None, None, :]).astype(jnp.float32)
        placed = jnp.einsum("skr,skih->rih", row_marks, products)
        return placed.reshape(NODE_DEV, FEATS)

    gathered = lax.map(one_block, (rows_all, cols_all, vals_all)).reshape(NODES, FEATS)
    combined = ((1.0 + eps_self[0]) * node_feats.astype(jnp.float32) + gathered).astype(jnp.bfloat16)
    pre = jnp.dot(combined, w_one, preferred_element_type=jnp.float32) + b_one.astype(jnp.float32)
    hidden = jnp.maximum(pre, 0.0).astype(jnp.bfloat16)
    layer_out = jnp.dot(hidden, w_two, preferred_element_type=jnp.float32) + b_two.astype(jnp.float32)
    return layer_out.astype(jnp.bfloat16)
```

```python
import functools

import jax
import jax.numpy as jnp
from jax import lax
from jax.experimental import pallas as pl
from jax.experimental.pallas import tpu as pltpu
from jax.sharding import PartitionSpec as P

MESH = pl.DeviceIdType.MESH
CHUNKS = 4
PIECES = 4
VMEM_LIMIT = 60 * 1024 * 1024


def gather_kernel(lines, n_feat, x_ref, w_ref, all_ref, wall_ref, send_sems, recv_sems, w_send, w_recv, own_sems):
    blk, feat = lax.axis_index("blk"), lax.axis_index("feat")
    line, side = lax.div(blk, 2), lax.rem(blk, 2)
    partner = line * 2 + (1 - side)
    mate = line + 1 - 2 * lax.rem(line, 2)
    mate_block = mate * 2 + side
    has_low, has_high = line > 0, line < lines - 1
    low, high = blk - 2, blk + 2
    depth = x_ref.shape[0] // CHUNKS
    half = CHUNKS // 2
    w_rows = w_ref.shape[0]

    barrier = pltpu.get_barrier_semaphore()
    pl.semaphore_signal(barrier, inc=1, device_id={"blk": partner}, device_id_type=MESH)
    for k in range(1, n_feat):
        pl.semaphore_signal(barrier, inc=1, device_id={"feat": lax.rem(feat + k, n_feat)}, device_id_type=MESH)

    @pl.when(has_low)
    def _():
        pl.semaphore_signal(barrier, inc=1, device_id={"blk": low}, device_id_type=MESH)

    @pl.when(has_high)
    def _():
        pl.semaphore_signal(barrier, inc=1, device_id={"blk": high}, device_id_type=MESH)

    pl.semaphore_wait(barrier, n_feat + has_low.astype(jnp.int32) + has_high.astype(jnp.int32))

    def piece(b, c):
        return all_ref.at[b, pl.ds(c * depth, depth), :]

    def copy(way, target, b, c, own=False):
        source = x_ref.at[pl.ds(c * depth, depth), :] if own else piece(b, c)
        return pltpu.make_async_remote_copy(
            src_ref=source,
            dst_ref=piece(b, c),
            send_sem=send_sems.at[way, b, c],
            recv_sem=recv_sems.at[b, c],
            device_id={"blk": target},
            device_id_type=MESH,
        )

    def arrive(b, c):
        copy(2, partner, b, c).wait_recv()

    def weight_copy(k):
        return pltpu.make_async_remote_copy(
            src_ref=w_ref,
            dst_ref=wall_ref.at[pl.ds(feat * w_rows, w_rows), :],
            send_sem=w_send.at[k - 1],
            recv_sem=w_recv.at[k - 1],
            device_id={"feat": lax.rem(feat + k, n_feat)},
            device_id_type=MESH,
        )

    def weight_arrive(k):
        rows = pl.ds(lax.rem(feat + n_feat - k, n_feat) * w_rows, w_rows)
        pltpu.make_async_remote_copy(
            src_ref=w_ref,
            dst_ref=wall_ref.at[rows, :],
            send_sem=w_send.at[k - 1],
            recv_sem=w_recv.at[k - 1],
            device_id={"feat": lax.rem(feat + k, n_feat)},
            device_id_type=MESH,
        ).wait_recv()

    def sends(act, c, b, lower_ok, upper_ok, across_ok, own=False):
        if lower_ok is not None:
            @pl.when(lower_ok)
            def _():
                act(copy(0, low, b, c, own))
        if upper_ok is not None:
            @pl.when(upper_ok)
            def _():
                act(copy(1, high, b, c, own))
        if across_ok is True:
            act(copy(2, partner, b, c, own))
        else:
            @pl.when(across_ok)
            def _():
                act(copy(2, partner, b, c, own))

    def extra(act, c):
        @pl.when(mate > line)
        def _():
            act(copy(1, high, partner, c))

        @pl.when(mate < line)
        def _():
            act(copy(0, low, partner, c))

    def plan(act, wait):
        for c in range(CHUNKS):
            sends(act, c, blk, has_low, has_high, True, own=True)
        for step in range(1, lines):
            for c in range(CHUNKS):
                for above in (True, False):
                    spot = line + step if above else line - step
                    b = spot * 2 + side

                    @pl.when(spot < lines if above else spot >= 0)
                    def _(b=b, above=above, c=c):
                        if wait:
                            arrive(b, c)
                        across = True if c >= half else b != mate_block
                        sends(act, c, b, has_low if above else None, None if above else has_high, across)
            if step == 1:
                for c in range(half):
                    if wait:
                        arrive(partner, c)
                    extra(act, c)

    own_copies = [
        pltpu.make_async_copy(x_ref, all_ref.at[blk], own_sems.at[0]),
        pltpu.make_async_copy(w_ref, wall_ref.at[pl.ds(feat * w_rows, w_rows), :], own_sems.at[1]),
    ]
    for own in own_copies:
        own.start()
    for k in range(1, n_feat):
        weight_copy(k).start()
    plan(lambda d: d.start(), True)
    for c in range(half, CHUNKS):
        arrive(partner, c)
    for step in range(1, lines):
        spot = lax.rem(line + step, lines)
        for c in range(CHUNKS):
            arrive(spot * 2 + (1 - side), c)
    for k in range(1, n_feat):
        weight_arrive(k)
    plan(lambda d: d.wait_send(), False)
    for k in range(1, n_feat):
        weight_copy(k).wait_send()
    for own in own_copies:
        own.wait()


def gather_all(lines, n_feat, x_t, w_pack):
    feats, rows = x_t.shape
    blocks = lines * 2
    return pl.pallas_call(
        functools.partial(gather_kernel, lines, n_feat),
        out_shape=(
            jax.ShapeDtypeStruct((blocks, feats, rows), x_t.dtype),
            jax.ShapeDtypeStruct((n_feat * w_pack.shape[0], w_pack.shape[1]), w_pack.dtype),
        ),
        in_specs=[pl.BlockSpec(memory_space=pltpu.VMEM)] * 2,
        out_specs=(pl.BlockSpec(memory_space=pl.ANY), pl.BlockSpec(memory_space=pltpu.VMEM)),
        scratch_shapes=[
            pltpu.SemaphoreType.DMA((3, blocks, CHUNKS)),
            pltpu.SemaphoreType.DMA((blocks, CHUNKS)),
            pltpu.SemaphoreType.DMA((n_feat - 1,)),
            pltpu.SemaphoreType.DMA((n_feat - 1,)),
            pltpu.SemaphoreType.DMA((2,)),
        ],
        compiler_params=pltpu.CompilerParams(
            collective_id=0, has_side_effects=True, vmem_limit_bytes=VMEM_LIMIT
        ),
    )(x_t, w_pack)


def aggregate_kernel(group, rows_ref, cols_ref, eps_ref, x_ref, tiles_ref, own_ref, out_ref, acc):
    src = pl.program_id(0)
    slots, tile = tiles_ref.shape[1], tiles_ref.shape[2]

    @pl.when(src == 0)
    def _():
        acc[...] = jnp.zeros_like(acc)

    @pl.loop(0, slots // group)
    def _(g):
        products = []
        for i in range(group):
            k = g * group + i
            lanes = pl.ds(pl.multiple_of(cols_ref[src, k] * tile, tile), tile)
            products.append(
                lax.dot_general(
                    x_ref[0, :, lanes], tiles_ref[0, k], (((1,), (1,)), ((), ())),
                    preferred_element_type=jnp.float32,
                )
            )
        for i in range(group):
            r = rows_ref[src, g * group + i]
            acc[r] = acc[r] + products[i]

    @pl.when(src == pl.num_programs(0) - 1)
    def _():
        scale = 1.0 + eps_ref[0]
        for r in range(acc.shape[0]):
            lanes = pl.ds(r * tile, tile)
            own = own_ref[:, lanes].astype(jnp.float32)
            out_ref[:, lanes] = (scale * own + acc[r]).astype(out_ref.dtype)


def aggregate(x_all, tile_rows, tile_cols, tile_values, eps_self, x_t):
    blocks, slots, tile, _ = tile_values.shape
    feats, rows = x_t.shape
    group = 8 if slots % 8 == 0 else 1
    return pl.pallas_call(
        functools.partial(aggregate_kernel, group),
        out_shape=jax.ShapeDtypeStruct((feats, rows), x_t.dtype),
        grid_spec=pltpu.PrefetchScalarGridSpec(
            num_scalar_prefetch=3,
            grid=(blocks,),
            in_specs=[
                pl.BlockSpec((1, feats, rows), lambda s, *_: (s, 0, 0)),
                pl.BlockSpec((1, slots, tile, tile), lambda s, *_: (s, 0, 0, 0)),
                pl.BlockSpec((feats, rows), lambda s, *_: (0, 0)),
            ],
            out_specs=pl.BlockSpec((feats, rows), lambda s, *_: (0, 0)),
            scratch_shapes=[pltpu.VMEM((rows // tile, feats, tile), jnp.float32)],
        ),
        compiler_params=pltpu.CompilerParams(vmem_limit_bytes=VMEM_LIMIT),
    )(tile_rows, tile_cols, eps_self, x_all, tile_values, x_t)


def perceptron_kernel(n_feat, comb_ref, w_ref, out_ref, rows_in, staged, in_send, in_recv, out_send, out_recv, own_sems):
    feat = lax.axis_index("feat")
    feats = comb_ref.shape[0]
    share = rows_in.shape[1]
    width = share // PIECES
    full = rows_in.shape[0]

    barrier = pltpu.get_barrier_semaphore()
    for k in range(1, n_feat):
        pl.semaphore_signal(barrier, inc=1, device_id={"feat": lax.rem(feat + k, n_feat)}, device_id_type=MESH)
    pl.semaphore_wait(barrier, n_feat - 1)

    def lanes_of(owner, c):
        return pl.ds(pl.multiple_of(owner * share + c * width, width), width)

    def rows_of(owner):
        return pl.ds(pl.multiple_of(owner * feats, feats), feats)

    def inward(k, c, receive=False):
        peer = lax.rem(feat + k, n_feat)
        writer = lax.rem(feat + n_feat - k, n_feat) if receive else feat
        return pltpu.make_async_remote_copy(
            src_ref=comb_ref.at[:, lanes_of(peer, c)],
            dst_ref=rows_in.at[rows_of(writer), pl.ds(c * width, width)],
            send_sem=in_send.at[k - 1, c],
            recv_sem=in_recv.at[k - 1, c],
            device_id={"feat": peer},
            device_id_type=MESH,
        )

    def outward(k, c, receive=False):
        peer = lax.rem(feat + k, n_feat)
        writer = lax.rem(feat + n_feat - k, n_feat) if receive else feat
        return pltpu.make_async_remote_copy(
            src_ref=staged.at[rows_of(peer), pl.ds(c * width, width)],
            dst_ref=out_ref.at[:, lanes_of(writer, c)],
            send_sem=out_send.at[k - 1, c],
            recv_sem=out_recv.at[k - 1, c],
            device_id={"feat": peer},
            device_id_type=MESH,
        )

    def own_in(c):
        return pltpu.make_async_copy(
            comb_ref.at[:, lanes_of(feat, c)], rows_in.at[rows_of(feat), pl.ds(c * width, width)], own_sems.at[0, c]
        )

    def own_out(c):
        return pltpu.make_async_copy(
            staged.at[rows_of(feat), pl.ds(c * width, width)], out_ref.at[:, lanes_of(feat, c)], own_sems.at[1, c]
        )

    for c in range(PIECES):
        for k in range(1, n_feat):
            inward(k, c).start()
        own_in(c).start()
    first = w_ref[:, :full]
    second = w_ref[:, full : 2 * full]
    bias_one = w_ref[:, 2 * full : 2 * full + 1].astype(jnp.float32)
    bias_two = w_ref[:, 2 * full + 1 : 2 * full + 2].astype(jnp.float32)
    for c in range(PIECES):
        own_in(c).wait()
        for k in range(1, n_feat):
            inward(k, c, True).wait_recv()
        at = pl.ds(c * width, width)
        pre = jnp.dot(first, rows_in[:, at], preferred_element_type=jnp.float32) + bias_one
        hidden = jnp.maximum(pre, 0.0).astype(jnp.bfloat16)
        out = lax.dot_general(second, hidden, (((0,), (0,)), ((), ())), preferred_element_type=jnp.float32)
        staged[:, at] = (out + bias_two).astype(staged.dtype)
        for k in range(1, n_feat):
            outward(k, c).start()
        own_out(c).start()
    for c in range(PIECES):
        for k in range(1, n_feat):
            outward(k, c, True).wait_recv()
        own_out(c).wait()
        for k in range(1, n_feat):
            inward(k, c).wait_send()
            outward(k, c).wait_send()


def perceptron(n_feat, comb_t, w_all):
    feats, rows = comb_t.shape
    share = rows // n_feat
    pair_sems = pltpu.SemaphoreType.DMA((n_feat - 1, PIECES))
    return pl.pallas_call(
        functools.partial(perceptron_kernel, n_feat),
        out_shape=jax.ShapeDtypeStruct((feats, rows), comb_t.dtype),
        in_specs=[pl.BlockSpec(memory_space=pltpu.VMEM)] * 2,
        out_specs=pl.BlockSpec(memory_space=pltpu.VMEM),
        scratch_shapes=[
            pltpu.VMEM((n_feat * feats, share), comb_t.dtype),
            pltpu.VMEM((n_feat * feats, share), comb_t.dtype),
            pair_sems, pair_sems, pair_sems, pair_sems,
            pltpu.SemaphoreType.DMA((2, PIECES)),
        ],
        compiler_params=pltpu.CompilerParams(
            collective_id=1, has_side_effects=True, vmem_limit_bytes=VMEM_LIMIT
        ),
    )(comb_t, w_all)


def solution(mesh):
    lines, n_feat = mesh.shape["blk"] // 2, mesh.shape["feat"]

    def on_device(node_feats, tile_rows, tile_cols, tile_values, eps_self, w_one, b_one, w_two, b_two):
        x_t = node_feats.T
        biases = jnp.stack([b_one, b_two], axis=1)
        biases = jnp.pad(biases, ((0, 0), (0, tile_values.shape[2] - 2)))
        w_pack = jnp.concatenate([w_one.T, w_two, biases], axis=1)
        x_all, w_all = gather_all(lines, n_feat, x_t, w_pack)
        comb_t = aggregate(x_all, tile_rows, tile_cols, tile_values, eps_self, x_t)
        return perceptron(n_feat, comb_t, w_all).T

    return jax.shard_map(
        on_device,
        mesh=mesh,
        in_specs=(
            P("blk", "feat"),
            P("blk", None),
            P("blk", None),
            P("blk", None, None, None),
            P(),
            P(None, "feat"),
            P("feat"),
            P("feat", None),
            P("feat"),
        ),
        out_specs=P("blk", "feat"),
        check_vma=False,
    )
```

```python
import functools

import jax
import jax.numpy as jnp
from jax import lax
from jax.experimental import pallas as pl
from jax.experimental.pallas import tpu as pltpu
from jax.sharding import PartitionSpec as P

MESH = pl.DeviceIdType.MESH
CHUNKS = 4
PIECES = 4
PARTS = 4
DEEP = 6
GROUP = 8
VMEM_LIMIT = 60 * 1024 * 1024


def gather_kernel(
    lines, n_feat, x_ref, w_ref, meta_ref, eps_ref, tiles_ref, comb_ref, wall_ref,
    all_ref, along, across_buf, tile_buf, sums, send_sems, recv_sems, w_send, w_recv, own_sems, tile_sems,
):
    blk, feat = lax.axis_index("blk"), lax.axis_index("feat")
    line, side = lax.div(blk, 2), lax.rem(blk, 2)
    partner = line * 2 + (1 - side)
    mate = line + 1 - 2 * lax.rem(line, 2)
    mate_block = mate * 2 + side
    has_low, has_high = line > 0, line < lines - 1
    low, high = blk - 2, blk + 2
    depth = x_ref.shape[0] // CHUNKS
    half = CHUNKS // 2
    w_rows = w_ref.shape[0]

    barrier = pltpu.get_barrier_semaphore()
    pl.semaphore_signal(barrier, inc=1, device_id={"blk": partner}, device_id_type=MESH)
    for k in range(1, n_feat):
        pl.semaphore_signal(barrier, inc=1, device_id={"feat": lax.rem(feat + k, n_feat)}, device_id_type=MESH)

    @pl.when(has_low)
    def _():
        pl.semaphore_signal(barrier, inc=1, device_id={"blk": low}, device_id_type=MESH)

    @pl.when(has_high)
    def _():
        pl.semaphore_signal(barrier, inc=1, device_id={"blk": high}, device_id_type=MESH)

    pl.semaphore_wait(barrier, n_feat + has_low.astype(jnp.int32) + has_high.astype(jnp.int32))

    def piece(b, c):
        return all_ref.at[b, pl.ds(c * depth, depth), :]

    def copy(way, target, b, c, own=False):
        source = x_ref.at[pl.ds(c * depth, depth), :] if own else piece(b, c)
        return pltpu.make_async_remote_copy(
            src_ref=source,
            dst_ref=piece(b, c),
            send_sem=send_sems.at[way, b, c],
            recv_sem=recv_sems.at[b, c],
            device_id={"blk": target},
            device_id_type=MESH,
        )

    def arrive(b, c):
        copy(2, partner, b, c).wait_recv()

    def weight_copy(k):
        return pltpu.make_async_remote_copy(
            src_ref=w_ref,
            dst_ref=wall_ref.at[pl.ds(feat * w_rows, w_rows), :],
            send_sem=w_send.at[k - 1],
            recv_sem=w_recv.at[k - 1],
            device_id={"feat": lax.rem(feat + k, n_feat)},
            device_id_type=MESH,
        )

    def weight_arrive(k):
        rows = pl.ds(lax.rem(feat + n_feat - k, n_feat) * w_rows, w_rows)
        pltpu.make_async_remote_copy(
            src_ref=w_ref,
            dst_ref=wall_ref.at[rows, :],
            send_sem=w_send.at[k - 1],
            recv_sem=w_recv.at[k - 1],
            device_id={"feat": lax.rem(feat + k, n_feat)},
            device_id_type=MESH,
        ).wait_recv()

    def sends(act, c, b, lower_ok, upper_ok, across_ok, own=False):
        if lower_ok is not None:
            @pl.when(lower_ok)
            def _():
                act(copy(0, low, b, c, own))
        if upper_ok is not None:
            @pl.when(upper_ok)
            def _():
                act(copy(1, high, b, c, own))
        if across_ok is True:
            act(copy(2, partner, b, c, own))
        else:
            @pl.when(across_ok)
            def _():
                act(copy(2, partner, b, c, own))

    def extra(act, c):
        @pl.when(mate > line)
        def _():
            act(copy(1, high, partner, c))

        @pl.when(mate < line)
        def _():
            act(copy(0, low, partner, c))

    def relay(act, wait, step, c):
        for above in (True, False):
            spot = line + step if above else line - step
            b = spot * 2 + side

            @pl.when(spot < lines if above else spot >= 0)
            def _(b=b, above=above):
                if wait:
                    arrive(b, c)
                across = True if c >= half else b != mate_block
                sends(act, c, b, has_low if above else None, None if above else has_high, across)

    slots, tile = tiles_ref.shape[1], tiles_ref.shape[2]
    part = slots // PARTS
    row_tiles = x_ref.shape[1] // tile
    by_distance = [sorted(range(lines), key=lambda o: (abs(o - l), o)) for l in range(lines)]

    def spot_of(j):
        spot = jnp.int32(0)
        for l in range(lines):
            spot = jnp.where(line == l, by_distance[l][j], spot)
        return spot

    jobs = [("along", 0)]
    for step in range(2, lines):
        jobs += [("along", step - 1), ("across", step - 2)]
    jobs += [("across", lines - 2), ("along", lines - 1), ("across", lines - 1)]
    sources = [spot_of(j) * 2 + (side if kind == "along" else 1 - side) for kind, j in jobs]

    def tile_copy(n):
        job, q = n // PARTS, n % PARTS
        return pltpu.make_async_copy(
            tiles_ref.at[sources[job], pl.ds(q * part, part)], tile_buf.at[n % DEEP], tile_sems.at[n % DEEP]
        )

    def stage(job):
        kind, j = jobs[job]
        b = sources[job]
        target = along if kind == "along" else across_buf
        for c in range(CHUNKS):
            if kind == "across" and (j > 0 or c >= half):
                arrive(b, c)

        @pl.loop(0, row_tiles)
        def _(t):
            lanes = pl.ds(pl.multiple_of(t * tile, tile), tile)
            target[t] = x_ref[:, lanes] if job == 0 else all_ref[b, :, lanes]

    total_parts = len(jobs) * PARTS

    def multiply(job, q):
        n = job * PARTS + q
        b = sources[job]
        if q == 0:
            stage(job)
        src = along if jobs[job][0] == "along" else across_buf
        tile_copy(n).wait()

        @pl.loop(0, part // GROUP)
        def _(g):
            products = []
            for i in range(GROUP):
                k = g * GROUP + i
                products.append(
                    lax.dot_general(
                        src[meta_ref[b, slots + q * part + k]], tile_buf[n % DEEP, k], (((1,), (1,)), ((), ())),
                        preferred_element_type=jnp.float32,
                    )
                )
            for i in range(GROUP):
                k = q * part + g * GROUP + i
                sums[row_tiles + k] = sums[meta_ref[b, k]] + products[i]

        if n + DEEP < total_parts:
            tile_copy(n + DEEP).start()
        if q == PARTS - 1 and job < len(jobs) - 1:
            @pl.loop(0, row_tiles)
            def _(r):
                sums[r] = sums[meta_ref[b, 2 * slots + r]]

    own_copy = pltpu.make_async_copy(w_ref, wall_ref.at[pl.ds(feat * w_rows, w_rows), :], own_sems.at[0])
    own_copy.start()
    for n in range(DEEP):
        tile_copy(n).start()
    for c in range(CHUNKS):
        sends(lambda d: d.start(), c, blk, has_low, has_high, True, own=True)
    for k in range(1, n_feat):
        weight_copy(k).start()
    scale = 1.0 + eps_ref[0]
    for r in range(row_tiles):
        sums[r] = scale * x_ref[:, r * tile : (r + 1) * tile].astype(jnp.float32)
    for q in range(PARTS):
        multiply(0, q)
    for step in range(1, lines):
        for c in range(CHUNKS):
            if step > 1:
                lo = c * 2 * PARTS // CHUNKS
                for u in range(lo, (c + 1) * 2 * PARTS // CHUNKS):
                    multiply(1 + 2 * (step - 2) + u // PARTS, u % PARTS)
            relay(lambda d: d.start(), True, step, c)
        if step == 1:
            for c in range(half):
                arrive(partner, c)
                extra(lambda d: d.start(), c)
    for job in range(len(jobs) - 3, len(jobs)):
        for q in range(PARTS):
            multiply(job, q)
    for r in range(row_tiles):
        comb_ref[:, r * tile : (r + 1) * tile] = sums[meta_ref[sources[-1], 2 * slots + r]].astype(comb_ref.dtype)
    for k in range(1, n_feat):
        weight_arrive(k)
    for c in range(CHUNKS):
        sends(lambda d: d.wait_send(), c, blk, has_low, has_high, True, own=True)
    for step in range(1, lines):
        for c in range(CHUNKS):
            relay(lambda d: d.wait_send(), False, step, c)
    for c in range(half):
        extra(lambda d: d.wait_send(), c)
    for k in range(1, n_feat):
        weight_copy(k).wait_send()
    own_copy.wait()


def gather_aggregate(lines, n_feat, x_t, w_pack, meta, eps_self, tile_values):
    feats, rows = x_t.shape
    blocks, slots, tile, _ = tile_values.shape
    row_tiles = rows // tile
    return pl.pallas_call(
        functools.partial(gather_kernel, lines, n_feat),
        out_shape=(
            jax.ShapeDtypeStruct((feats, rows), x_t.dtype),
            jax.ShapeDtypeStruct((n_feat * w_pack.shape[0], w_pack.shape[1]), w_pack.dtype),
        ),
        in_specs=[
            pl.BlockSpec(memory_space=pltpu.VMEM),
            pl.BlockSpec(memory_space=pltpu.VMEM),
            pl.BlockSpec(memory_space=pltpu.SMEM),
            pl.BlockSpec(memory_space=pltpu.SMEM),
            pl.BlockSpec(memory_space=pl.ANY),
        ],
        out_specs=(pl.BlockSpec(memory_space=pltpu.VMEM), pl.BlockSpec(memory_space=pltpu.VMEM)),
        scratch_shapes=[
            pltpu.VMEM((blocks, feats, rows), x_t.dtype),
            pltpu.VMEM((row_tiles, feats, tile), x_t.dtype),
            pltpu.VMEM((row_tiles, feats, tile), x_t.dtype),
            pltpu.VMEM((DEEP, slots // PARTS, tile, tile), tile_values.dtype),
            pltpu.VMEM((row_tiles + slots, feats, tile), jnp.float32),
            pltpu.SemaphoreType.DMA((3, blocks, CHUNKS)),
            pltpu.SemaphoreType.DMA((blocks, CHUNKS)),
            pltpu.SemaphoreType.DMA((n_feat - 1,)),
            pltpu.SemaphoreType.DMA((n_feat - 1,)),
            pltpu.SemaphoreType.DMA((1,)),
            pltpu.SemaphoreType.DMA((DEEP,)),
        ],
        compiler_params=pltpu.CompilerParams(
            collective_id=0, has_side_effects=True, vmem_limit_bytes=VMEM_LIMIT
        ),
    )(x_t, w_pack, meta, eps_self, tile_values)


def chain_meta(tile_rows, tile_cols, row_tiles):
    slots = tile_rows.shape[1]
    slot = jnp.arange(slots, dtype=jnp.int32)
    same = tile_rows[:, :, None] == tile_rows[:, None, :]
    earlier = jnp.max(jnp.where(same & (slot[None, None, :] < slot[None, :, None]), slot[None, None, :], -1), axis=2)
    prev = jnp.where(earlier >= 0, row_tiles + earlier, tile_rows)
    row = jnp.arange(row_tiles, dtype=jnp.int32)
    hit = tile_rows[:, None, :] == row[None, :, None]
    final = jnp.max(jnp.where(hit, slot[None, None, :], -1), axis=2)
    last = jnp.where(final >= 0, row_tiles + final, row[None, :])
    return jnp.concatenate([prev, tile_cols, last], axis=1)


def perceptron_kernel(n_feat, comb_ref, w_ref, out_ref, rows_in, staged, in_send, in_recv, out_send, out_recv, own_sems):
    feat = lax.axis_index("feat")
    feats = comb_ref.shape[0]
    share = rows_in.shape[1]
    width = share // PIECES
    full = rows_in.shape[0]

    barrier = pltpu.get_barrier_semaphore()
    for k in range(1, n_feat):
        pl.semaphore_signal(barrier, inc=1, device_id={"feat": lax.rem(feat + k, n_feat)}, device_id_type=MESH)
    pl.semaphore_wait(barrier, n_feat - 1)

    def lanes_of(owner, c):
        return pl.ds(pl.multiple_of(owner * share + c * width, width), width)

    def rows_of(owner):
        return pl.ds(pl.multiple_of(owner * feats, feats), feats)

    def inward(k, c, receive=False):
        peer = lax.rem(feat + k, n_feat)
        writer = lax.rem(feat + n_feat - k, n_feat) if receive else feat
        return pltpu.make_async_remote_copy(
            src_ref=comb_ref.at[:, lanes_of(peer, c)],
            dst_ref=rows_in.at[rows_of(writer), pl.ds(c * width, width)],
            send_sem=in_send.at[k - 1, c],
            recv_sem=in_recv.at[k - 1, c],
            device_id={"feat": peer},
            device_id_type=MESH,
        )

    def outward(k, c, receive=False):
        peer = lax.rem(feat + k, n_feat)
        writer = lax.rem(feat + n_feat - k, n_feat) if receive else feat
        return pltpu.make_async_remote_copy(
            src_ref=staged.at[rows_of(peer), pl.ds(c * width, width)],
            dst_ref=out_ref.at[:, lanes_of(writer, c)],
            send_sem=out_send.at[k - 1, c],
            recv_sem=out_recv.at[k - 1, c],
            device_id={"feat": peer},
            device_id_type=MESH,
        )

    def own_in(c):
        return pltpu.make_async_copy(
            comb_ref.at[:, lanes_of(feat, c)], rows_in.at[rows_of(feat), pl.ds(c * width, width)], own_sems.at[0, c]
        )

    def own_out(c):
        return pltpu.make_async_copy(
            staged.at[rows_of(feat), pl.ds(c * width, width)], out_ref.at[:, lanes_of(feat, c)], own_sems.at[1, c]
        )

    for c in range(PIECES):
        for k in range(1, n_feat):
            inward(k, c).start()
        own_in(c).start()
    first = w_ref[:, :full]
    second = w_ref[:, full : 2 * full]
    bias_one = w_ref[:, 2 * full : 2 * full + 1].astype(jnp.float32)
    bias_two = w_ref[:, 2 * full + 1 : 2 * full + 2].astype(jnp.float32)
    for c in range(PIECES):
        own_in(c).wait()
        for k in range(1, n_feat):
            inward(k, c, True).wait_recv()
        at = pl.ds(c * width, width)
        pre = jnp.dot(first, rows_in[:, at], preferred_element_type=jnp.float32) + bias_one
        hidden = jnp.maximum(pre, 0.0).astype(jnp.bfloat16)
        out = lax.dot_general(second, hidden, (((0,), (0,)), ((), ())), preferred_element_type=jnp.float32)
        staged[:, at] = (out + bias_two).astype(staged.dtype)
        for k in range(1, n_feat):
            outward(k, c).start()
        own_out(c).start()
    for c in range(PIECES):
        for k in range(1, n_feat):
            outward(k, c, True).wait_recv()
        own_out(c).wait()
        for k in range(1, n_feat):
            inward(k, c).wait_send()
            outward(k, c).wait_send()


def perceptron(n_feat, comb_t, w_all):
    feats, rows = comb_t.shape
    share = rows // n_feat
    pair_sems = pltpu.SemaphoreType.DMA((n_feat - 1, PIECES))
    return pl.pallas_call(
        functools.partial(perceptron_kernel, n_feat),
        out_shape=jax.ShapeDtypeStruct((feats, rows), comb_t.dtype),
        in_specs=[pl.BlockSpec(memory_space=pltpu.VMEM)] * 2,
        out_specs=pl.BlockSpec(memory_space=pltpu.VMEM),
        scratch_shapes=[
            pltpu.VMEM((n_feat * feats, share), comb_t.dtype),
            pltpu.VMEM((n_feat * feats, share), comb_t.dtype),
            pair_sems, pair_sems, pair_sems, pair_sems,
            pltpu.SemaphoreType.DMA((2, PIECES)),
        ],
        compiler_params=pltpu.CompilerParams(
            collective_id=1, has_side_effects=True, vmem_limit_bytes=VMEM_LIMIT
        ),
    )(comb_t, w_all)


def solution(mesh):
    lines, n_feat = mesh.shape["blk"] // 2, mesh.shape["feat"]

    def on_device(node_feats, tile_rows, tile_cols, tile_values, eps_self, w_one, b_one, w_two, b_two):
        x_t = node_feats.T
        biases = jnp.stack([b_one, b_two], axis=1)
        biases = jnp.pad(biases, ((0, 0), (0, tile_values.shape[2] - 2)))
        w_pack = jnp.concatenate([w_one.T, w_two, biases], axis=1)
        meta = chain_meta(tile_rows, tile_cols, x_t.shape[1] // tile_values.shape[2])
        comb_t, w_all = gather_aggregate(lines, n_feat, x_t, w_pack, meta, eps_self, tile_values)
        return perceptron(n_feat, comb_t, w_all).T

    return jax.shard_map(
        on_device,
        mesh=mesh,
        in_specs=(
            P("blk", "feat"),
            P("blk", None),
            P("blk", None),
            P("blk", None, None, None),
            P(),
            P(None, "feat"),
            P("feat"),
            P("feat", None),
            P("feat"),
        ),
        out_specs=P("blk", "feat"),
        check_vma=False,
    )
```

```python
import functools

import jax
import jax.numpy as jnp
from jax import lax
from jax.experimental import pallas as pl
from jax.experimental.pallas import tpu as pltpu
from jax.sharding import PartitionSpec as P

MESH = pl.DeviceIdType.MESH
CHUNKS = 4
PIECES = 4
PARTS = 4
DEEP = 6
GROUP = 8
VMEM_LIMIT = 60 * 1024 * 1024


def gather_kernel(
    lines, n_feat, x_ref, w_ref, meta_ref, eps_ref, tiles_ref, comb_ref, wall_ref,
    all_ref, along, across_buf, tile_buf, sums, send_sems, recv_sems, w_send, w_recv, own_sems, tile_sems,
):
    blk, feat = lax.axis_index("blk"), lax.axis_index("feat")
    line, side = lax.div(blk, 2), lax.rem(blk, 2)
    partner = line * 2 + (1 - side)
    mate = line + 1 - 2 * lax.rem(line, 2)
    mate_block = mate * 2 + side
    has_low, has_high = line > 0, line < lines - 1
    low, high = blk - 2, blk + 2
    depth = x_ref.shape[0] // CHUNKS
    half = CHUNKS // 2
    w_rows = w_ref.shape[0]

    barrier = pltpu.get_barrier_semaphore()
    pl.semaphore_signal(barrier, inc=1, device_id={"blk": partner}, device_id_type=MESH)
    for k in range(1, n_feat):
        pl.semaphore_signal(barrier, inc=1, device_id={"feat": lax.rem(feat + k, n_feat)}, device_id_type=MESH)

    @pl.when(has_low)
    def _():
        pl.semaphore_signal(barrier, inc=1, device_id={"blk": low}, device_id_type=MESH)

    @pl.when(has_high)
    def _():
        pl.semaphore_signal(barrier, inc=1, device_id={"blk": high}, device_id_type=MESH)

    pl.semaphore_wait(barrier, n_feat + has_low.astype(jnp.int32) + has_high.astype(jnp.int32))

    def piece(b, c):
        return all_ref.at[b, pl.ds(c * depth, depth), :]

    def copy(way, target, b, c, own=False):
        source = x_ref.at[pl.ds(c * depth, depth), :] if own else piece(b, c)
        return pltpu.make_async_remote_copy(
            src_ref=source,
            dst_ref=piece(b, c),
            send_sem=send_sems.at[way, b, c],
            recv_sem=recv_sems.at[b, c],
            device_id={"blk": target},
            device_id_type=MESH,
        )

    def arrive(b, c):
        copy(2, partner, b, c).wait_recv()

    def weight_copy(k):
        return pltpu.make_async_remote_copy(
            src_ref=w_ref,
            dst_ref=wall_ref.at[pl.ds(feat * w_rows, w_rows), :],
            send_sem=w_send.at[k - 1],
            recv_sem=w_recv.at[k - 1],
            device_id={"feat": lax.rem(feat + k, n_feat)},
            device_id_type=MESH,
        )

    def weight_arrive(k):
        rows = pl.ds(lax.rem(feat + n_feat - k, n_feat) * w_rows, w_rows)
        pltpu.make_async_remote_copy(
            src_ref=w_ref,
            dst_ref=wall_ref.at[rows, :],
            send_sem=w_send.at[k - 1],
            recv_sem=w_recv.at[k - 1],
            device_id={"feat": lax.rem(feat + k, n_feat)},
            device_id_type=MESH,
        ).wait_recv()

    def sends(act, c, b, lower_ok, upper_ok, across_ok, own=False):
        if lower_ok is not None:
            @pl.when(lower_ok)
            def _():
                act(copy(0, low, b, c, own))
        if upper_ok is not None:
            @pl.when(upper_ok)
            def _():
                act(copy(1, high, b, c, own))
        if across_ok is True:
            act(copy(2, partner, b, c, own))
        else:
            @pl.when(across_ok)
            def _():
                act(copy(2, partner, b, c, own))

    def extra(act, c):
        @pl.when(mate > line)
        def _():
            act(copy(1, high, partner, c))

        @pl.when(mate < line)
        def _():
            act(copy(0, low, partner, c))

    def relay(act, wait, step, c):
        for above in (True, False):
            spot = line + step if above else line - step
            b = spot * 2 + side

            @pl.when(spot < lines if above else spot >= 0)
            def _(b=b, above=above):
                if wait:
                    arrive(b, c)
                across = True if c >= half else b != mate_block
                sends(act, c, b, has_low if above else None, None if above else has_high, across)

    slots, tile = tiles_ref.shape[1], tiles_ref.shape[2]
    part = slots // PARTS
    row_tiles = x_ref.shape[1] // tile
    by_distance = [sorted(range(lines), key=lambda o: (abs(o - l), o)) for l in range(lines)]

    def spot_of(j):
        spot = jnp.int32(0)
        for l in range(lines):
            spot = jnp.where(line == l, by_distance[l][j], spot)
        return spot

    jobs = [("along", 0)]
    for step in range(2, lines):
        jobs += [("along", step - 1), ("across", step - 2)]
    jobs += [("across", lines - 2), ("along", lines - 1), ("across", lines - 1)]
    sources = [spot_of(j) * 2 + (side if kind == "along" else 1 - side) for kind, j in jobs]

    def tile_copy(n):
        job, q = n // PARTS, n % PARTS
        return pltpu.make_async_copy(
            tiles_ref.at[sources[job], pl.ds(q * part, part)], tile_buf.at[n % DEEP], tile_sems.at[n % DEEP]
        )

    def stage(job):
        kind, j = jobs[job]
        b = sources[job]
        target = along if kind == "along" else across_buf
        for c in range(CHUNKS):
            if kind == "across" and (j > 0 or c >= half):
                arrive(b, c)

        @pl.loop(0, row_tiles)
        def _(t):
            lanes = pl.ds(pl.multiple_of(t * tile, tile), tile)
            target[t] = x_ref[:, lanes] if job == 0 else all_ref[b, :, lanes]

    total_parts = len(jobs) * PARTS

    def multiply(job, q):
        n = job * PARTS + q
        b = sources[job]
        if q == 0:
            stage(job)
        src = along if jobs[job][0] == "along" else across_buf
        tile_copy(n).wait()

        @pl.loop(0, part // GROUP)
        def _(g):
            products = []
            for i in range(GROUP):
                k = g * GROUP + i
                products.append(
                    lax.dot_general(
                        src[meta_ref[b, slots + q * part + k]], tile_buf[n % DEEP, k], (((1,), (1,)), ((), ())),
                        preferred_element_type=jnp.float32,
                    )
                )
            for i in range(GROUP):
                k = q * part + g * GROUP + i
                sums[row_tiles + k] = sums[meta_ref[b, k]] + products[i]

        if n + DEEP < total_parts:
            tile_copy(n + DEEP).start()
        if q == PARTS - 1 and job < len(jobs) - 1:
            @pl.loop(0, row_tiles)
            def _(r):
                sums[r] = sums[meta_ref[b, 2 * slots + r]]

    own_copy = pltpu.make_async_copy(w_ref, wall_ref.at[pl.ds(feat * w_rows, w_rows), :], own_sems.at[0])
    own_copy.start()
    for n in range(DEEP):
        tile_copy(n).start()
    for c in range(CHUNKS):
        sends(lambda d: d.start(), c, blk, has_low, has_high, True, own=True)
    for k in range(1, n_feat):
        weight_copy(k).start()
    scale = 1.0 + eps_ref[0]
    for r in range(row_tiles):
        sums[r] = scale * x_ref[:, r * tile : (r + 1) * tile].astype(jnp.float32)
    for q in range(PARTS):
        multiply(0, q)
    done = PARTS
    for step in range(1, lines):
        for c in range(CHUNKS):
            if step == lines - 1 and step > 1:
                before = (2 * step - 3) * PARTS + 3 * PARTS // 2
                upto = before + c * (3 * PARTS // 2) // (CHUNKS - 1)
            else:
                upto = (2 * step - 3) * PARTS + (c + 1) * 2 * PARTS // CHUNKS
            while done < upto:
                multiply(done // PARTS, done % PARTS)
                done += 1
            relay(lambda d: d.start(), True, step, c)
        if step == 1:
            for c in range(half):
                arrive(partner, c)
                extra(lambda d: d.start(), c)
    while done < total_parts:
        multiply(done // PARTS, done % PARTS)
        done += 1
    for r in range(row_tiles):
        comb_ref[:, r * tile : (r + 1) * tile] = sums[meta_ref[sources[-1], 2 * slots + r]].astype(comb_ref.dtype)
    for k in range(1, n_feat):
        weight_arrive(k)
    for c in range(CHUNKS):
        sends(lambda d: d.wait_send(), c, blk, has_low, has_high, True, own=True)
    for step in range(1, lines):
        for c in range(CHUNKS):
            relay(lambda d: d.wait_send(), False, step, c)
    for c in range(half):
        extra(lambda d: d.wait_send(), c)
    for k in range(1, n_feat):
        weight_copy(k).wait_send()
    own_copy.wait()


def gather_aggregate(lines, n_feat, x_t, w_pack, meta, eps_self, tile_values):
    feats, rows = x_t.shape
    blocks, slots, tile, _ = tile_values.shape
    row_tiles = rows // tile
    return pl.pallas_call(
        functools.partial(gather_kernel, lines, n_feat),
        out_shape=(
            jax.ShapeDtypeStruct((feats, rows), x_t.dtype),
            jax.ShapeDtypeStruct((n_feat * w_pack.shape[0], w_pack.shape[1]), w_pack.dtype),
        ),
        in_specs=[
            pl.BlockSpec(memory_space=pltpu.VMEM),
            pl.BlockSpec(memory_space=pltpu.VMEM),
            pl.BlockSpec(memory_space=pltpu.SMEM),
            pl.BlockSpec(memory_space=pltpu.SMEM),
            pl.BlockSpec(memory_space=pl.ANY),
        ],
        out_specs=(pl.BlockSpec(memory_space=pltpu.VMEM), pl.BlockSpec(memory_space=pltpu.VMEM)),
        scratch_shapes=[
            pltpu.VMEM((blocks, feats, rows), x_t.dtype),
            pltpu.VMEM((row_tiles, feats, tile), x_t.dtype),
            pltpu.VMEM((row_tiles, feats, tile), x_t.dtype),
            pltpu.VMEM((DEEP, slots // PARTS, tile, tile), tile_values.dtype),
            pltpu.VMEM((row_tiles + slots, feats, tile), jnp.float32),
            pltpu.SemaphoreType.DMA((3, blocks, CHUNKS)),
            pltpu.SemaphoreType.DMA((blocks, CHUNKS)),
            pltpu.SemaphoreType.DMA((n_feat - 1,)),
            pltpu.SemaphoreType.DMA((n_feat - 1,)),
            pltpu.SemaphoreType.DMA((1,)),
            pltpu.SemaphoreType.DMA((DEEP,)),
        ],
        compiler_params=pltpu.CompilerParams(
            collective_id=0, has_side_effects=True, vmem_limit_bytes=VMEM_LIMIT
        ),
    )(x_t, w_pack, meta, eps_self, tile_values)


def chain_meta(tile_rows, tile_cols, row_tiles):
    slots = tile_rows.shape[1]
    slot = jnp.arange(slots, dtype=jnp.int32)
    same = tile_rows[:, :, None] == tile_rows[:, None, :]
    earlier = jnp.max(jnp.where(same & (slot[None, None, :] < slot[None, :, None]), slot[None, None, :], -1), axis=2)
    prev = jnp.where(earlier >= 0, row_tiles + earlier, tile_rows)
    row = jnp.arange(row_tiles, dtype=jnp.int32)
    hit = tile_rows[:, None, :] == row[None, :, None]
    final = jnp.max(jnp.where(hit, slot[None, None, :], -1), axis=2)
    last = jnp.where(final >= 0, row_tiles + final, row[None, :])
    return jnp.concatenate([prev, tile_cols, last], axis=1)


def perceptron_kernel(n_feat, comb_ref, w_ref, out_ref, rows_in, staged, in_send, in_recv, out_send, out_recv, own_sems):
    feat = lax.axis_index("feat")
    feats = comb_ref.shape[0]
    share = rows_in.shape[1]
    width = share // PIECES
    full = rows_in.shape[0]

    barrier = pltpu.get_barrier_semaphore()
    for k in range(1, n_feat):
        pl.semaphore_signal(barrier, inc=1, device_id={"feat": lax.rem(feat + k, n_feat)}, device_id_type=MESH)
    pl.semaphore_wait(barrier, n_feat - 1)

    def lanes_of(owner, c):
        return pl.ds(pl.multiple_of(owner * share + c * width, width), width)

    def rows_of(owner):
        return pl.ds(pl.multiple_of(owner * feats, feats), feats)

    def inward(k, c, receive=False):
        peer = lax.rem(feat + k, n_feat)
        writer = lax.rem(feat + n_feat - k, n_feat) if receive else feat
        return pltpu.make_async_remote_copy(
            src_ref=comb_ref.at[:, lanes_of(peer, c)],
            dst_ref=rows_in.at[rows_of(writer), pl.ds(c * width, width)],
            send_sem=in_send.at[k - 1, c],
            recv_sem=in_recv.at[k - 1, c],
            device_id={"feat": peer},
            device_id_type=MESH,
        )

    def outward(k, c, receive=False):
        peer = lax.rem(feat + k, n_feat)
        writer = lax.rem(feat + n_feat - k, n_feat) if receive else feat
        return pltpu.make_async_remote_copy(
            src_ref=staged.at[rows_of(peer), pl.ds(c * width, width)],
            dst_ref=out_ref.at[:, lanes_of(writer, c)],
            send_sem=out_send.at[k - 1, c],
            recv_sem=out_recv.at[k - 1, c],
            device_id={"feat": peer},
            device_id_type=MESH,
        )

    def own_in(c):
        return pltpu.make_async_copy(
            comb_ref.at[:, lanes_of(feat, c)], rows_in.at[rows_of(feat), pl.ds(c * width, width)], own_sems.at[0, c]
        )

    def own_out(c):
        return pltpu.make_async_copy(
            staged.at[rows_of(feat), pl.ds(c * width, width)], out_ref.at[:, lanes_of(feat, c)], own_sems.at[1, c]
        )

    for c in range(PIECES):
        for k in range(1, n_feat):
            inward(k, c).start()
        own_in(c).start()
    first = w_ref[:, :full]
    second = w_ref[:, full : 2 * full]
    bias_one = w_ref[:, 2 * full : 2 * full + 1].astype(jnp.float32)
    bias_two = w_ref[:, 2 * full + 1 : 2 * full + 2].astype(jnp.float32)
    for c in range(PIECES):
        own_in(c).wait()
        for k in range(1, n_feat):
            inward(k, c, True).wait_recv()
        at = pl.ds(c * width, width)
        pre = jnp.dot(first, rows_in[:, at], preferred_element_type=jnp.float32) + bias_one
        hidden = jnp.maximum(pre, 0.0).astype(jnp.bfloat16)
        out = lax.dot_general(second, hidden, (((0,), (0,)), ((), ())), preferred_element_type=jnp.float32)
        staged[:, at] = (out + bias_two).astype(staged.dtype)
        for k in range(1, n_feat):
            outward(k, c).start()
        own_out(c).start()
    for c in range(PIECES):
        for k in range(1, n_feat):
            outward(k, c, True).wait_recv()
        own_out(c).wait()
        for k in range(1, n_feat):
            inward(k, c).wait_send()
            outward(k, c).wait_send()


def perceptron(n_feat, comb_t, w_all):
    feats, rows = comb_t.shape
    share = rows // n_feat
    pair_sems = pltpu.SemaphoreType.DMA((n_feat - 1, PIECES))
    return pl.pallas_call(
        functools.partial(perceptron_kernel, n_feat),
        out_shape=jax.ShapeDtypeStruct((feats, rows), comb_t.dtype),
        in_specs=[pl.BlockSpec(memory_space=pltpu.VMEM)] * 2,
        out_specs=pl.BlockSpec(memory_space=pltpu.VMEM),
        scratch_shapes=[
            pltpu.VMEM((n_feat * feats, share), comb_t.dtype),
            pltpu.VMEM((n_feat * feats, share), comb_t.dtype),
            pair_sems, pair_sems, pair_sems, pair_sems,
            pltpu.SemaphoreType.DMA((2, PIECES)),
        ],
        compiler_params=pltpu.CompilerParams(
            collective_id=1, has_side_effects=True, vmem_limit_bytes=VMEM_LIMIT
        ),
    )(comb_t, w_all)


def solution(mesh):
    lines, n_feat = mesh.shape["blk"] // 2, mesh.shape["feat"]

    def on_device(node_feats, tile_rows, tile_cols, tile_values, eps_self, w_one, b_one, w_two, b_two):
        x_t = node_feats.T
        biases = jnp.stack([b_one, b_two], axis=1)
        biases = jnp.pad(biases, ((0, 0), (0, tile_values.shape[2] - 2)))
        w_pack = jnp.concatenate([w_one.T, w_two, biases], axis=1)
        meta = chain_meta(tile_rows, tile_cols, x_t.shape[1] // tile_values.shape[2])
        comb_t, w_all = gather_aggregate(lines, n_feat, x_t, w_pack, meta, eps_self, tile_values)
        return perceptron(n_feat, comb_t, w_all).T

    return jax.shard_map(
        on_device,
        mesh=mesh,
        in_specs=(
            P("blk", "feat"),
            P("blk", None),
            P("blk", None),
            P("blk", None, None, None),
            P(),
            P(None, "feat"),
            P("feat"),
            P("feat", None),
            P("feat"),
        ),
        out_specs=P("blk", "feat"),
        check_vma=False,
    )
```
